256 devices in a mesh: batch: 2 (over core), neuron: 128 (over z, y, x).
Axes of the slice: x: 4, y: 4, z: 8, core: 2. Of those that a mesh axis runs over, the one named last changes fastest.
Arguments:
- images: bfloat16 [32, 65536], P('batch', 'neuron'), parts along dimension 0, may hold values from 0 to 32
- tile_weights: bfloat16 [2, 16384, 128, 128], P(None, 'neuron'), may hold values from -0.375 to 0.375
- tile_blocks: int32 [2, 16384, 2], P(None, 'neuron'), may hold values from 0 to 511, as said below
- tile_count: int32 [2, 128], P(None, 'neuron'), may hold values from 96 to 128, as said below
- bias: float32 [2, 65536], P(None, 'neuron'), may hold values from -48 to 48
Outputs:
- activity: bfloat16 [32, 65536], P('batch', 'neuron'), parts along dimension 0
The draws below stay inside these ranges and needn't reach their ends.
There are 2 independent parts, one for each index of `batch`. The reference program is written for one: setup_inputs(seed, part) draws one part's arguments, and reference() takes and returns one part's arrays. A program takes and returns all parts, laid end to end along the dimension named above; an argument that names none is the same for every part. Nothing has to cross between parts.
Inputs may be any that keep to these rules, and one draw needn't show every extreme that they name: Slots 0 to tile_count[l, d] - 1 of device d are live in layer l; in every layer one device has all 128 live. `tile_blocks`: entry [l, d * 128 + s, :] is the row block and column block of slot s of device d. Within one device and layer the column blocks are all different, and at most 2 of them lie among the 4 column blocks of any one neuron device; in every layer the column blocks of some neuron device get exactly 2 live slots from every device.
All inputs are finite; a program needn't handle non-finite values.
Results may differ from the reference program's by a relative error of at most 0.0033.
Values may be sent and summed in bfloat16 or wider, within the bound.
No kernel may reach another device: no remote copies, remote signals or barrier semaphores. Data moves between devices by JAX's collectives and lax.ppermute only.
A program may use at most 64 MiB of HBM per device.

```python
import jax
import jax.numpy as jnp
from jax import lax

NEURONS = 65536
BLOCK = 128
LAYERS = 2
IMAGES = 16
TILES_DEV = 128
BLK_DEV = 4
SLOT_MOST = 2
N_NEURON = 128


def distinct_order(key, shape):
    scores = jax.random.randint(key, shape, 0, 65536) * shape[-1] + jnp.arange(shape[-1], dtype=jnp.int32)
    return jnp.argsort(scores, axis=-1, stable=True).astype(jnp.int32)


def draw_tile_blocks(key, part):
    base_key = jax.random.fold_in(key, 23)
    key_rows, key_owner, key_common, key_offset, key_shuffle = jax.random.split(base_key, 5)
    row_ids = jax.random.randint(key_rows, (LAYERS, N_NEURON, TILES_DEV), 0, NEURONS // BLOCK)
    owner_order = distinct_order(key_owner, (LAYERS, N_NEURON, N_NEURON))
    common = jax.random.randint(key_common, (LAYERS, 1, 1), 0, N_NEURON)
    slot_ids = jnp.arange(TILES_DEV, dtype=jnp.int32)
    groups = jnp.broadcast_to(slot_ids // SLOT_MOST, (LAYERS, N_NEURON, TILES_DEV))
    chosen = jnp.take_along_axis(owner_order, groups, axis=-1)
    owners = (chosen - owner_order[:, :, :1] + common) % N_NEURON
    offsets = jax.random.randint(key_offset, (LAYERS, N_NEURON, N_NEURON), 0, BLK_DEV)
    shifted = jnp.take_along_axis(offsets, groups, axis=-1)
    local_ids = (shifted + slot_ids % SLOT_MOST) % BLK_DEV
    col_ids = owners * BLK_DEV + local_ids
    tail_order = distinct_order(key_shuffle, (LAYERS, N_NEURON, TILES_DEV - SLOT_MOST))
    tail = jnp.take_along_axis(col_ids[:, :, SLOT_MOST:], tail_order, axis=-1)
    col_ids = jnp.concatenate([col_ids[:, :, :SLOT_MOST], tail], axis=-1)
    stacked = jnp.stack([row_ids, col_ids], axis=-1)
    return stacked.reshape(LAYERS, N_NEURON * TILES_DEV, 2).astype(jnp.int32)


def draw_tile_count(key, part):
    base_key = jax.random.fold_in(key, 11)
    key_first, key_busy = jax.random.split(base_key, 2)
    counts = jax.random.randint(key_first, (LAYERS, N_NEURON), TILES_DEV - TILES_DEV // 4, TILES_DEV + 1)
    busiest = jax.random.randint(key_busy, (LAYERS, 1), 0, N_NEURON)
    counts = jnp.where(jnp.arange(N_NEURON, dtype=jnp.int32)[None, :] == busiest, TILES_DEV, counts)
    return counts.astype(jnp.int32)


def steps_of(rng, extent, cuts, least, top_value):
    loudness, own = 1.0, jax.random.fold_in(rng, 6)
    for axis_at, parts in cuts:
        heights = jnp.exp(jax.random.uniform(jax.random.fold_in(own, axis_at), (parts,), jnp.float32, least / len(cuts), top_value / len(cuts)))
        loudness = loudness * jnp.repeat(heights, extent[axis_at] // parts).reshape([-1 if axis == axis_at else 1 for axis in range(len(extent))])
    return loudness


def gaussian(stream_key, extent, spread, reach, cuts=(), kind=jnp.bfloat16):
    values = spread * jax.random.normal(stream_key, extent, jnp.float32)
    if cuts:
        values = values * steps_of(stream_key, extent, cuts, -0.22, 0.18)
    return jnp.clip(values, -reach, reach).astype(kind)


def setup_inputs(seed: int = 0, part: int = 0) -> dict:
    key_list = jax.random.split(jax.random.key(seed), 6)
    own_keys = jax.random.split(jax.random.fold_in(key_list[5], part), 6)
    return {
        "images": jnp.clip(32.0 * jax.random.uniform(own_keys[0], (IMAGES, NEURONS), jnp.float32) ** steps_of(own_keys[0], (IMAGES, NEURONS), ((1, 128),), -0.2, 0.2), 0.0, 32.0).astype(jnp.bfloat16),
        "tile_weights": gaussian(key_list[1], (LAYERS, N_NEURON * TILES_DEV, BLOCK, BLOCK), (2 * BLOCK) ** -0.5, 0.375, ((1, 128),)),
        "tile_blocks": draw_tile_blocks(jax.random.fold_in(key_list[5], 71), part),
        "tile_count": draw_tile_count(jax.random.fold_in(key_list[5], 71), part),
        "bias": gaussian(key_list[4], (LAYERS, NEURONS), 8.0, 48.0, ((1, 128),), jnp.float32),
    }


CEILING = 32.0


def reference(images, tile_weights, tile_blocks, tile_count, bias):
    all_blocks = NEURONS // BLOCK
    activity = images
    for layer_index in range(LAYERS):
        block_view = activity.reshape(IMAGES, all_blocks, BLOCK).astype(jnp.float32)

        def device_terms(totals, pieces):
            weights, blocks, live_count = pieces
            picked = jnp.take(block_view, blocks[:, 0], axis=1)
            products = jnp.einsum("bsk,skn->sbn", picked, weights.astype(jnp.float32))
            usable = jnp.arange(TILES_DEV, dtype=jnp.int32) < live_count
            products = jnp.where(usable[:, None, None], products, jnp.zeros_like(products))
            return totals.at[blocks[:, 1]].add(products), live_count

        initial = jnp.zeros((all_blocks, IMAGES, BLOCK), jnp.float32)
        totals, unused = lax.scan(
            device_terms,
            initial,
            (
                tile_weights[layer_index].reshape(N_NEURON, TILES_DEV, BLOCK, BLOCK),
                tile_blocks[layer_index].reshape(N_NEURON, TILES_DEV, 2),
                tile_count[layer_index],
            ),
        )
        summed = jnp.transpose(totals, (1, 0, 2)).reshape(IMAGES, NEURONS)
        activity = jnp.clip(summed + bias[layer_index][None, :], 0.0, CEILING).astype(jnp.bfloat16)
    return activity
```

```python
import functools

import jax
import jax.numpy as jnp
from jax import lax
from jax.experimental import pallas as pl
from jax.experimental.pallas import tpu as pltpu
from jax.sharding import Mesh
from jax.sharding import PartitionSpec as P

NEURON = ("neuron_0", "neuron_1", "neuron_2")
PLANE = ("neuron_1", "neuron_2")
CEILING = 32.0
WIRE = jnp.float16

SMEM = functools.partial(pl.BlockSpec, memory_space=pltpu.SMEM)
VMEM = functools.partial(pl.BlockSpec, memory_space=pltpu.VMEM)
ANY = functools.partial(pl.BlockSpec, memory_space=pl.ANY)


def label_kernel(planes, heights, own, slots, blocks_ref, count_ref, label_ref, target_ref, fill_ref):
    room = slots // planes * 2
    for layer in range(blocks_ref.shape[0]):
        for p in range(planes):
            fill_ref[p] = 0
        for t in range(planes * room):
            label_ref[t // room, layer * room + t % room] = heights * own

        def place(s, carry):
            col = blocks_ref[layer, 1, s]
            owner = col // own
            p = owner % planes
            k = fill_ref[p]

            @pl.when(s < count_ref[layer, 0])
            def _():
                fill_ref[p] = k + 1
                label_ref[p, layer * room + k] = (owner // planes) * own + col % own
                target_ref[layer, s] = p * room + k

            return carry

        lax.fori_loop(0, slots, place, 0)


def product_kernel(layer, chunks, sure, blocks_ref, target_ref, count_ref, acts_ref, weights_ref, out_ref, held_ref, sems):
    planes, heights = acts_ref.shape[0], acts_ref.shape[1]
    slots, width = held_ref.shape[0], held_ref.shape[1]
    per = slots // chunks
    own = acts_ref.shape[3] // width
    copies = [
        pltpu.make_async_copy(
            weights_ref.at[layer, pl.ds(c * per, per)], held_ref.at[pl.ds(c * per, per)], sems.at[c]
        )
        for c in range(chunks)
    ]
    for copy in copies:
        copy.start()
    out_ref[...] = jnp.zeros_like(out_ref)

    def one(s):
        row = blocks_ref[layer, 0, s]
        owner = row // own
        lane = pl.multiple_of((row % own) * width, width)
        picked = acts_ref[owner % planes, owner // planes, :, pl.ds(lane, width)]
        product = jnp.dot(picked, held_ref[s], preferred_element_type=jnp.float32)
        out_ref[target_ref[layer, s]] = product.astype(out_ref.dtype)

    for c in range(chunks):
        copies[c].wait()
        for i in range(per):
            s = c * per + i
            if s < sure:
                one(s)
            else:
                pl.when(s < count_ref[layer, 0])(functools.partial(one, s))


def last_kernel(layer, got_ref, bias_ref, out_ref):
    heights, own, rows, width = got_ref.shape
    for b in range(own):
        total = got_ref[0, b]
        for z in range(1, heights):
            total += got_ref[z, b]
        total += bias_ref[layer : layer + 1, b * width : (b + 1) * width]
        done = jnp.clip(total, 0.0, CEILING).astype(out_ref.dtype)
        for z in range(out_ref.shape[0]):
            out_ref[z, :, b * width : (b + 1) * width] = done


def exchanged(value, axes):
    return lax.all_to_all(value, axes, split_axis=0, concat_axis=0, tiled=True)


def local(images, tile_weights, tile_blocks, tile_count, bias):
    layers, slots, width, _ = tile_weights.shape
    rows, local_width = images.shape
    own = local_width // width
    planes = lax.axis_size(PLANE)
    heights = lax.axis_size(NEURON[0])
    room = slots // planes * 2
    chunks = 8
    sure = slots - slots // 4
    blocks = tile_blocks.transpose(0, 2, 1)

    labels, targets = pl.pallas_call(
        functools.partial(label_kernel, planes, heights, own, slots),
        out_shape=(
            jax.ShapeDtypeStruct((planes, layers * room), jnp.int32),
            jax.ShapeDtypeStruct((layers, slots), jnp.int32),
        ),
        in_specs=[SMEM(), SMEM()],
        out_specs=(SMEM(), SMEM()),
        scratch_shapes=[pltpu.SMEM((planes,), jnp.int32)],
        name="labels",
    )(blocks, tile_count)
    labels = exchanged(labels, PLANE)
    dense = jnp.arange(heights * own, dtype=jnp.int32)[:, None]

    copies = jnp.broadcast_to(images[None], (heights, rows, local_width))
    for layer in range(layers):
        column = exchanged(copies, NEURON[0])
        spread = jnp.broadcast_to(column[None], (planes, heights, rows, local_width))
        acts = exchanged(spread, PLANE)
        outgoing = pl.pallas_call(
            functools.partial(product_kernel, layer, chunks, sure),
            out_shape=jax.ShapeDtypeStruct((planes * room, rows, width), jnp.float32),
            in_specs=[SMEM(), SMEM(), SMEM(), VMEM(), ANY()],
            out_specs=VMEM(),
            scratch_shapes=[
                pltpu.VMEM((slots, width, width), jnp.bfloat16),
                pltpu.SemaphoreType.DMA((chunks,)),
            ],
            name="products",
        )(blocks, targets, tile_count, acts.reshape(planes, heights, rows, local_width), tile_weights)
        got = exchanged(outgoing.astype(WIRE), PLANE)
        chosen = (labels[:, layer * room : (layer + 1) * room].reshape(1, -1) == dense).astype(jnp.float32)
        middle = jnp.einsum(
            "or,rbn->obn", chosen, got.astype(jnp.float32), precision=lax.Precision.HIGH
        )
        ended = exchanged(middle.astype(WIRE), NEURON[0]).astype(jnp.float32)
        out_copies = heights if layer + 1 < layers else 1
        copies = pl.pallas_call(
            functools.partial(last_kernel, layer),
            out_shape=jax.ShapeDtypeStruct((out_copies, rows, local_width), jnp.bfloat16),
            in_specs=[VMEM(), VMEM()],
            out_specs=VMEM(),
            name="last",
        )(ended.reshape(heights, own, rows, width), bias)
    return copies[0]


def solution(mesh):
    split = Mesh(
        mesh.devices.reshape(mesh.shape["batch"], 8, 4, 4),
        ("batch", "neuron_0", "neuron_1", "neuron_2"),
    )
    in_specs = (
        P("batch", NEURON),
        P(None, NEURON, None, None),
        P(None, NEURON, None),
        P(None, NEURON),
        P(None, NEURON),
    )
    out_specs = P("batch", NEURON)
    return jax.shard_map(local, mesh=split, in_specs=in_specs, out_specs=out_specs, check_vma=False)
```

```python
import functools

import jax
import jax.numpy as jnp
from jax import lax
from jax.experimental import pallas as pl
from jax.experimental.pallas import tpu as pltpu
from jax.sharding import Mesh
from jax.sharding import PartitionSpec as P

NEURON = ("neuron_0", "neuron_1", "neuron_2")
PLANE = ("neuron_1", "neuron_2")
CEILING = 32.0
WIRE = jnp.float16
ROOM = 16 * 2**20
WIDE = 46 * 2**20

SMEM = functools.partial(pl.BlockSpec, memory_space=pltpu.SMEM)
VMEM = functools.partial(pl.BlockSpec, memory_space=pltpu.VMEM)
HBM = functools.partial(pl.BlockSpec, memory_space=pltpu.HBM)


def cost(flops):
    return pl.CostEstimate(flops=flops, bytes_accessed=0, transcendentals=0)


def routes(tile_blocks, tile_count, own):
    nz, ny, nx = (lax.axis_size(axis) for axis in NEURON)
    layers, slots, _ = tile_blocks.shape
    planes, half, room = ny * nx, nz // 2, slots // (ny * nx) * 2
    rows, cols = tile_blocks[:, :, 0], tile_blocks[:, :, 1]
    ids = jnp.arange(slots, dtype=jnp.int32)
    live = ids[None, :] < tile_count

    holder = rows // own
    away_y = (lax.axis_index(NEURON[1]) + ny - (holder // nx) % ny) % ny
    away_x = (lax.axis_index(NEURON[2]) + nx - holder % nx) % nx
    z = holder // planes
    low = (away_y * nx + away_x) * half + z
    high = (away_x * ny + away_y) * half + z - half + planes * half
    source = jnp.where(live, jnp.where(z < half, low, high), planes * nz) * own + rows % own

    owner = cols // own
    plane = owner % planes
    ahead = (plane[:, :, None] == plane[:, None, :]) & (ids[None, None, :] < ids[None, :, None])
    target = jnp.where(live, plane * room + jnp.sum(ahead.astype(jnp.int32), axis=2), 0)
    label = jnp.where(live, (owner // planes) * own + cols % own + 1, 0)
    place = jnp.arange(planes * room, dtype=jnp.int32)
    here = target[:, None, :] == place[None, :, None]
    table = jnp.sum(jnp.where(here, label[:, None, :], 0), axis=2)
    return source, target, table.reshape(layers, planes, room)


def product_kernel(layer, chunks, source_ref, target_ref, *refs):
    *piece_refs, weights_ref, bias_ref, out_ref, bias_out_ref, acts_ref, held_ref, sems, bias_sem = refs
    slots, width = held_ref.shape[0], held_ref.shape[1]
    per = slots // chunks
    own = acts_ref.shape[2] // width
    order = list(reversed(range(chunks)))
    copies = {
        c: pltpu.make_async_copy(
            weights_ref.at[layer, pl.ds(c * per, per)], held_ref.at[pl.ds(c * per, per)], sems.at[c]
        )
        for c in order
    }
    for c in order:
        copies[c].start()
    bias_copy = pltpu.make_async_copy(bias_ref, bias_out_ref, bias_sem)
    bias_copy.start()
    at = 0
    for piece_ref in piece_refs:
        size = piece_ref.shape[0]
        acts_ref[at : at + size] = piece_ref[...]
        at += size
    acts_ref[at] = jnp.zeros(acts_ref.shape[1:], acts_ref.dtype)
    out_ref[...] = jnp.zeros_like(out_ref)
    for c in order:
        copies[c].wait()
        for s in reversed(range(c * per, (c + 1) * per)):
            source = source_ref[layer, s]
            lane = pl.multiple_of((source % own) * width, width)
            picked = acts_ref[source // own, :, pl.ds(lane, width)]
            out_ref[target_ref[layer, s]] = jnp.dot(picked, held_ref[s], preferred_element_type=jnp.float32)
    bias_copy.wait()


def last_kernel(layer, got_ref, bias_ref, out_ref):
    heights, own, rows, width = got_ref.shape
    for b in range(own):
        total = got_ref[0, b]
        for z in range(1, heights):
            total += got_ref[z, b]
        total += bias_ref[layer : layer + 1, b * width : (b + 1) * width]
        done = jnp.clip(total, 0.0, CEILING).astype(out_ref.dtype)
        for z in range(out_ref.shape[0]):
            out_ref[z, :, b * width : (b + 1) * width] = done


def exchanged(value, axes):
    return lax.all_to_all(value, axes, split_axis=0, concat_axis=0, tiled=True)


def shifted(value, axis):
    size = lax.axis_size(axis)
    shift = lambda k: lax.ppermute(value, axis, [(i, (i + k) % size) for i in range(size)])
    moved = {k: shift(k) for k in sorted(range(1, size), key=lambda k: min(k, size - k))}
    return [value] + [moved[k] for k in range(1, size)]


def local(images, tile_weights, tile_blocks, tile_count, bias):
    layers, slots, width, _ = tile_weights.shape
    rows, local_width = images.shape
    own = local_width // width
    nz, ny, nx = (lax.axis_size(axis) for axis in NEURON)
    planes = ny * nx
    room = slots // planes * 2
    chunks = 8
    small = pltpu.CompilerParams(vmem_limit_bytes=ROOM)

    sources, targets, tables = routes(tile_blocks, tile_count, own)
    labels = exchanged(tables.transpose(1, 0, 2).reshape(planes, layers * room), PLANE)
    dense = jnp.arange(1, nz * own + 1, dtype=jnp.int32)[:, None]

    copies = jnp.broadcast_to(images[None], (nz, rows, local_width))
    for layer in range(layers):
        column = exchanged(copies, NEURON[0])
        low = jnp.concatenate(shifted(column[: nz // 2], PLANE[1]))
        high = jnp.concatenate(shifted(column[nz // 2 :], PLANE[0]))
        pieces = shifted(low, PLANE[0]) + shifted(high, PLANE[1])
        outgoing, near_bias = pl.pallas_call(
            functools.partial(product_kernel, layer, chunks),
            out_shape=(
                jax.ShapeDtypeStruct((planes * room, rows, width), jnp.float32),
                jax.ShapeDtypeStruct(bias.shape, bias.dtype),
            ),
            in_specs=[SMEM(), SMEM()] + [VMEM()] * len(pieces) + [HBM(), HBM()],
            out_specs=(VMEM(), VMEM()),
            scratch_shapes=[
                pltpu.VMEM((planes * nz + 1, rows, local_width), jnp.bfloat16),
                pltpu.VMEM((slots, width, width), jnp.bfloat16),
                pltpu.SemaphoreType.DMA((chunks,)),
                pltpu.SemaphoreType.DMA,
            ],
            compiler_params=pltpu.CompilerParams(vmem_limit_bytes=WIDE),
            cost_estimate=cost(2 * slots * rows * width * width),
            name="products",
        )(sources, targets, *pieces, tile_weights, bias)
        got = exchanged(outgoing.astype(WIRE), PLANE)
        chosen = (labels[:, layer * room : (layer + 1) * room].reshape(1, -1) == dense).astype(jnp.float32)
        middle = jnp.einsum("or,rbn->obn", chosen, got.astype(jnp.float32), precision=lax.Precision.HIGH)
        ended = exchanged(middle.astype(WIRE), NEURON[0]).astype(jnp.float32)
        out_copies = nz if layer + 1 < layers else 1
        copies = pl.pallas_call(
            functools.partial(last_kernel, layer),
            out_shape=jax.ShapeDtypeStruct((out_copies, rows, local_width), jnp.bfloat16),
            in_specs=[VMEM(), VMEM()],
            out_specs=VMEM(),
            compiler_params=small,
            name="last",
        )(ended.reshape(nz, own, rows, width), near_bias)
    return copies[0]


def solution(mesh):
    split = Mesh(
        mesh.devices.reshape(mesh.shape["batch"], 8, 4, 4),
        ("batch", "neuron_0", "neuron_1", "neuron_2"),
    )
    in_specs = (
        P("batch", NEURON),
        P(None, NEURON, None, None),
        P(None, NEURON, None),
        P(None, NEURON),
        P(None, NEURON),
    )
    out_specs = P("batch", NEURON)
    return jax.shard_map(local, mesh=split, in_specs=in_specs, out_specs=out_specs, check_vma=False)
```

```python
import jax
import jax.numpy as jnp
from jax import lax
from jax.sharding import Mesh
from jax.sharding import PartitionSpec as P

NEURON = ("neuron_0", "neuron_1", "neuron_2")
HEIGHT = NEURON[0]
PLANE = NEURON[1:]
CEILING = 32.0
WIRE = jnp.float16


def exchanged(value, axes):
    return lax.all_to_all(value, axes, split_axis=0, concat_axis=0, tiled=True)


def local(images, tile_weights, tile_blocks, tile_count, bias):
    layers, slots, width, _ = tile_weights.shape
    rows, local_width = images.shape
    own = local_width // width
    heights = lax.axis_size(HEIGHT)
    planes = lax.axis_size(PLANE)
    each = rows // planes
    held = planes * own
    every = heights * held
    block_ids = jnp.arange(every, dtype=jnp.int32)

    live = jnp.arange(slots, dtype=jnp.int32)[None, :] < tile_count
    routes = jnp.where(live[:, None, :], tile_blocks.transpose(0, 2, 1), -1)
    facts = jnp.concatenate(
        [routes.reshape(layers * 2, slots).astype(jnp.float32), bias.reshape(layers * own, width)], axis=0
    )
    opening = jnp.concatenate(
        [
            images.reshape(planes, each * own, width).astype(jnp.float32),
            jnp.broadcast_to(facts[None], (planes,) + facts.shape),
        ],
        axis=1,
    )
    opened = exchanged(opening, PLANE)
    state = opened[:, :own].reshape(held, width).astype(jnp.bfloat16)
    routes = opened[:, own : own + layers * 2].astype(jnp.int32)
    biases = opened[:, own + layers * 2 :]

    for layer in range(layers):
        spread = jnp.broadcast_to(state[None], (heights, held, width)).reshape(every, width)
        acts = exchanged(spread, HEIGHT)
        from_rows = (routes[:, layer * 2].reshape(-1)[:, None] == block_ids[None, :]).astype(jnp.bfloat16)
        wanted = jnp.dot(from_rows, acts, preferred_element_type=jnp.float32).astype(jnp.bfloat16)
        picked = exchanged(wanted.reshape(planes, slots, width), PLANE)
        products = jnp.einsum("isk,skn->isn", picked, tile_weights[layer], preferred_element_type=jnp.float32)
        returned = exchanged(products.astype(WIRE), PLANE)
        to_cols = (block_ids[:, None] == routes[:, layer * 2 + 1].reshape(-1)[None, :]).astype(jnp.float32)
        partial = jnp.dot(
            to_cols, returned.reshape(planes * slots, width).astype(jnp.float32), precision=lax.Precision.HIGH
        )
        ended = exchanged(partial.astype(WIRE), HEIGHT).reshape(heights, held, width)
        summed = jnp.sum(ended.astype(jnp.float32), axis=0)
        summed += biases[:, layer * own : (layer + 1) * own].reshape(held, width)
        state = jnp.clip(summed, 0.0, CEILING).astype(jnp.bfloat16)
    return exchanged(state.reshape(planes, own, width), PLANE).reshape(rows, local_width)


def solution(mesh):
    split = Mesh(
        mesh.devices.reshape(mesh.shape["batch"], 8, 4, 4),
        ("batch", "neuron_0", "neuron_1", "neuron_2"),
    )
    in_specs = (
        P("batch", NEURON),
        P(None, NEURON, None, None),
        P(None, NEURON, None),
        P(None, NEURON),
        P(None, NEURON),
    )
    out_specs = P("batch", NEURON)
    return jax.shard_map(local, mesh=split, in_specs=in_specs, out_specs=out_specs, check_vma=False)
```

```python
import functools

import jax
import jax.numpy as jnp
from jax import lax
from jax.experimental import pallas as pl
from jax.experimental.pallas import tpu as pltpu
from jax.sharding import Mesh
from jax.sharding import PartitionSpec as P

NEURON = ("neuron_0", "neuron_1", "neuron_2")
HEIGHT = NEURON[0]
PLANE = NEURON[1:]
CEILING = 32.0
WIRE = jnp.float16


def exchanged(value, axes):
    return lax.all_to_all(value, axes, split_axis=0, concat_axis=0, tiled=True)


def opening_kernel(count_ref, images_ref, blocks_ref, bias_ref, out_ref):
    layers, sides, slots = blocks_ref.shape
    planes, _, width = out_ref.shape
    own = images_ref.shape[1] // width
    ids = lax.broadcasted_iota(jnp.int32, (1, slots), 1)
    for b in range(own):
        out_ref[:, b, :] = images_ref[:, b * width : (b + 1) * width].astype(jnp.float32)
    at = own
    for layer in range(layers):
        live = ids < count_ref[0, layer]
        for side in range(sides):
            route = jnp.where(live, blocks_ref[layer, side : side + 1, :], -1).astype(jnp.float32)
            out_ref[:, at, :] = jnp.broadcast_to(route, (planes, slots))
            at += 1
    for layer in range(layers):
        for b in range(own):
            part = bias_ref[layer : layer + 1, b * width : (b + 1) * width]
            out_ref[:, at, :] = jnp.broadcast_to(part, (planes, width))
            at += 1


def ranks(match):
    size = match.shape[-1]
    ids = jnp.arange(size, dtype=jnp.int32)
    return jnp.sum((match[..., None, :] & (ids[None, :] < ids[:, None])).astype(jnp.int32), axis=-1)


def local(images, tile_weights, tile_blocks, tile_count, bias):
    layers, slots, width, _ = tile_weights.shape
    rows, local_width = images.shape
    own = local_width // width
    heights = lax.axis_size(HEIGHT)
    planes = lax.axis_size(PLANE)
    me = lax.axis_index(PLANE)
    held = planes * own
    every = heights * held
    room = slots // planes * 2
    block_ids = jnp.arange(every, dtype=jnp.int32)

    opening = pl.pallas_call(
        opening_kernel,
        out_shape=jax.ShapeDtypeStruct((planes, own + layers * 2 + layers * own, width), jnp.float32),
        in_specs=[pl.BlockSpec(memory_space=pltpu.SMEM)] + [pl.BlockSpec(memory_space=pltpu.VMEM)] * 3,
        out_specs=pl.BlockSpec(memory_space=pltpu.VMEM),
        name="opening",
    )(tile_count.T, images, tile_blocks.transpose(0, 2, 1), bias)
    opened = exchanged(opening, PLANE)
    state = opened[:, :own].reshape(held, width).astype(jnp.bfloat16)
    routes = opened[:, own : own + layers * 2].astype(jnp.int32)
    biases = opened[:, own + layers * 2 :]

    own_cols = jnp.where(
        jnp.arange(slots, dtype=jnp.int32) < tile_count[layers - 1, 0], tile_blocks[layers - 1, :, 1], -every
    )
    plane = (own_cols // own) % planes
    same = (plane[:, None] == plane[None, :]) & (own_cols >= 0)[None, :]
    earlier = jnp.arange(slots)[None, :] < jnp.arange(slots)[:, None]
    target = plane * room + jnp.sum((same & earlier).astype(jnp.int32), axis=1)
    target = jnp.where(own_cols >= 0, target, -1)
    cols = routes[:, layers * 2 - 1]
    mine = (cols >= 0) & ((cols // own) % planes == me)
    place = jnp.where(mine, ranks(mine), -1)
    label = jnp.where(mine, (cols // held) * own + cols % own, 0) + 1
    here = place[:, None, :] == jnp.arange(room, dtype=jnp.int32)[None, :, None]
    labels = jnp.sum(jnp.where(here, label[:, None, :], 0), axis=2).reshape(-1)

    packing = (jnp.arange(planes * room, dtype=jnp.int32)[:, None] == target[None, :]).astype(jnp.float32)
    chosen = (jnp.arange(1, heights * own + 1, dtype=jnp.int32)[:, None] == labels[None, :]).astype(jnp.float32)
    last_bias = bias[layers - 1]

    for layer in range(layers):
        spread = jnp.broadcast_to(state[None], (heights, held, width)).reshape(every, width)
        acts = exchanged(spread, HEIGHT)
        if layer == 0:
            acts, packing, chosen, last_bias = lax.optimization_barrier((acts, packing, chosen, last_bias))
        from_rows = (routes[:, layer * 2].reshape(-1)[:, None] == block_ids[None, :]).astype(jnp.bfloat16)
        wanted = jnp.dot(from_rows, acts, preferred_element_type=jnp.float32).astype(jnp.bfloat16)
        picked = exchanged(wanted.reshape(planes, slots, width), PLANE)
        products = jnp.einsum("isk,skn->isn", picked, tile_weights[layer], preferred_element_type=jnp.float32)
        products = products.astype(WIRE)
        if layer + 1 == layers:
            break
        cols = routes[:, layer * 2 + 1]
        returned = exchanged(products, PLANE)
        to_cols = (block_ids[:, None] == cols.reshape(-1)[None, :]).astype(jnp.float32)
        partial = jnp.dot(
            to_cols, returned.reshape(planes * slots, width).astype(jnp.float32), precision=lax.Precision.HIGH
        )
        ended = exchanged(partial.astype(WIRE), HEIGHT).reshape(heights, held, width)
        summed = jnp.sum(ended.astype(jnp.float32), axis=0)
        summed += biases[:, layer * own : (layer + 1) * own].reshape(held, width)
        state = jnp.clip(summed, 0.0, CEILING).astype(jnp.bfloat16)

    packed = jnp.einsum("ts,isn->tin", packing, products.astype(jnp.float32), precision=lax.Precision.HIGH)
    got = exchanged(packed.astype(WIRE), PLANE)
    middle = jnp.einsum("or,rin->oin", chosen, got.astype(jnp.float32), precision=lax.Precision.HIGH)
    ended = exchanged(middle.astype(WIRE), HEIGHT).reshape(heights, own, rows, width)
    summed = jnp.sum(ended.astype(jnp.float32), axis=0).transpose(1, 0, 2).reshape(rows, local_width)
    return jnp.clip(summed + last_bias[None, :], 0.0, CEILING).astype(jnp.bfloat16)


def solution(mesh):
    split = Mesh(
        mesh.devices.reshape(mesh.shape["batch"], 8, 4, 4),
        ("batch", "neuron_0", "neuron_1", "neuron_2"),
    )
    in_specs = (
        P("batch", NEURON),
        P(None, NEURON, None, None),
        P(None, NEURON, None),
        P(None, NEURON),
        P(None, NEURON),
    )
    out_specs = P("batch", NEURON)
    return jax.shard_map(local, mesh=split, in_specs=in_specs, out_specs=out_specs, check_vma=False)
```

```python
import functools

import jax
import jax.numpy as jnp
from jax import lax
from jax.experimental import pallas as pl
from jax.experimental.pallas import tpu as pltpu
from jax.sharding import Mesh
from jax.sharding import PartitionSpec as P

NEURON = ("neuron_0", "neuron_1", "neuron_2")
HEIGHT = NEURON[0]
PLANE = NEURON[1:]
CEILING = 32.0
WIRE = jnp.float16


def exchanged(value, axes):
    return lax.all_to_all(value, axes, split_axis=0, concat_axis=0, tiled=True)


def opening_kernel(count_ref, images_ref, blocks_ref, bias_ref, out_ref):
    layers, sides, slots = blocks_ref.shape
    planes, _, width = out_ref.shape
    own = images_ref.shape[1] // width
    ids = lax.broadcasted_iota(jnp.int32, (1, slots), 1)
    for b in range(own):
        out_ref[:, b, :] = images_ref[:, b * width : (b + 1) * width].astype(jnp.float32)
    at = own
    for layer in range(layers):
        live = ids < count_ref[0, layer]
        for side in range(sides):
            route = jnp.where(live, blocks_ref[layer, side : side + 1, :], -1).astype(jnp.float32)
            out_ref[:, at, :] = jnp.broadcast_to(route, (planes, slots))
            at += 1
    for layer in range(layers):
        for b in range(own):
            part = bias_ref[layer : layer + 1, b * width : (b + 1) * width]
            out_ref[:, at, :] = jnp.broadcast_to(part, (planes, width))
            at += 1


def ranks(match):
    size = match.shape[-1]
    ids = jnp.arange(size, dtype=jnp.int32)
    return jnp.sum((match[..., None, :] & (ids[None, :] < ids[:, None])).astype(jnp.int32), axis=-1)


def local(images, tile_weights, tile_blocks, tile_count, bias):
    layers, slots, width, _ = tile_weights.shape
    rows, local_width = images.shape
    own = local_width // width
    heights = lax.axis_size(HEIGHT)
    planes = lax.axis_size(PLANE)
    me = lax.axis_index(PLANE)
    held = planes * own
    every = heights * held
    room = slots // planes * 2
    block_ids = jnp.arange(every, dtype=jnp.int32)

    opening = pl.pallas_call(
        opening_kernel,
        out_shape=jax.ShapeDtypeStruct((planes, own + layers * 2 + layers * own, width), jnp.float32),
        in_specs=[pl.BlockSpec(memory_space=pltpu.SMEM)] + [pl.BlockSpec(memory_space=pltpu.VMEM)] * 3,
        out_specs=pl.BlockSpec(memory_space=pltpu.VMEM),
        name="opening",
    )(tile_count.T, images, tile_blocks.transpose(0, 2, 1), bias)
    opened = exchanged(opening, PLANE)
    state = opened[:, :own].reshape(held, width).astype(jnp.bfloat16)
    routes = opened[:, own : own + layers * 2].astype(jnp.int32)
    biases = opened[:, own + layers * 2 :]

    own_row = lax.dynamic_index_in_dim(opened, me, axis=0, keepdims=False)
    own_cols = own_row[own + layers * 2 - 1].astype(jnp.int32)
    last_bias = own_row[own + layers * 2 + (layers - 1) * own :]
    plane = (own_cols // own) % planes
    same = (plane[:, None] == plane[None, :]) & (own_cols >= 0)[None, :]
    earlier = jnp.arange(slots)[None, :] < jnp.arange(slots)[:, None]
    target = plane * room + jnp.sum((same & earlier).astype(jnp.int32), axis=1)
    target = jnp.where(own_cols >= 0, target, -1)
    cols = routes[:, layers * 2 - 1]
    mine = (cols >= 0) & ((cols // own) % planes == me)
    place = jnp.where(mine, ranks(mine), -1)
    label = jnp.where(mine, (cols // held) * own + cols % own, 0) + 1
    here = place[:, None, :] == jnp.arange(room, dtype=jnp.int32)[None, :, None]
    labels = jnp.sum(jnp.where(here, label[:, None, :], 0), axis=2).reshape(-1)

    packing = (jnp.arange(planes * room, dtype=jnp.int32)[:, None] == target[None, :]).astype(jnp.float32)
    chosen = (jnp.arange(1, heights * own + 1, dtype=jnp.int32)[:, None] == labels[None, :]).astype(jnp.float32)

    for layer in range(layers):
        spread = jnp.broadcast_to(state[None], (heights, held, width)).reshape(every, width)
        acts = exchanged(spread, HEIGHT)
        if layer == 0:
            acts, packing, chosen, last_bias = lax.optimization_barrier((acts, packing, chosen, last_bias))
        from_rows = (routes[:, layer * 2].reshape(-1)[:, None] == block_ids[None, :]).astype(jnp.bfloat16)
        wanted = jnp.dot(from_rows, acts, preferred_element_type=jnp.float32).astype(jnp.bfloat16)
        picked = exchanged(wanted.reshape(planes, slots, width), PLANE)
        products = jnp.einsum("isk,skn->isn", picked, tile_weights[layer], preferred_element_type=jnp.float32)
        products = products.astype(WIRE)
        if layer + 1 == layers:
            break
        cols = routes[:, layer * 2 + 1]
        returned = exchanged(products, PLANE)
        to_cols = (block_ids[:, None] == cols.reshape(-1)[None, :]).astype(jnp.float32)
        partial = jnp.dot(
            to_cols, returned.reshape(planes * slots, width).astype(jnp.float32), precision=lax.Precision.HIGH
        )
        ended = exchanged(partial.astype(WIRE), HEIGHT).reshape(heights, held, width)
        summed = jnp.sum(ended.astype(jnp.float32), axis=0)
        summed += biases[:, layer * own : (layer + 1) * own].reshape(held, width)
        state = jnp.clip(summed, 0.0, CEILING).astype(jnp.bfloat16)

    packed = jnp.einsum("ts,isn->tin", packing, products.astype(jnp.float32), precision=lax.Precision.HIGH)
    got = exchanged(packed.astype(WIRE), PLANE)
    middle = jnp.einsum("or,rin->oin", chosen, got.astype(jnp.float32), precision=lax.Precision.HIGH)
    ended = exchanged(middle.astype(WIRE), HEIGHT).reshape(heights, own, rows, width)
    summed = jnp.sum(ended.astype(jnp.float32), axis=0) + last_bias[:, None, :]
    activity = jnp.clip(summed, 0.0, CEILING).astype(jnp.bfloat16)
    return activity.transpose(1, 0, 2).reshape(rows, local_width)


def solution(mesh):
    split = Mesh(
        mesh.devices.reshape(mesh.shape["batch"], 8, 4, 4),
        ("batch", "neuron_0", "neuron_1", "neuron_2"),
    )
    in_specs = (
        P("batch", NEURON),
        P(None, NEURON, None, None),
        P(None, NEURON, None),
        P(None, NEURON),
        P(None, NEURON),
    )
    out_specs = P("batch", NEURON)
    return jax.shard_map(local, mesh=split, in_specs=in_specs, out_specs=out_specs, check_vma=False)
```
